512 devices in a mesh: grp: 8 (over z), row: 64 (over y, x, core).
Axes of the slice: x: 4, y: 8, z: 8, core: 2. Of those that a mesh axis runs over, the one named last changes fastest.
Arguments:
- tiles: bfloat16 [3072, 512, 512], P(('grp', 'row')), may hold values from -0.15625 to 0.15625
- tile_row: int32 [3072], P(('grp', 'row')), may hold values from 0 to 1023, as said below
- tile_col: int32 [3072], P(('grp', 'row')), may hold values from 0 to 1023, as said below
- tile_count: int32 [512], P(('grp', 'row')), may hold values from 3 to 6, as said below
- q_block: bfloat16 [524288, 256], P(('grp', 'row')), may hold values from -80 to 80
Outputs:
- q_next: float32 [524288, 256], P(('grp', 'row'))
The draws below stay inside these ranges and needn't reach their ends.
Inputs may be any that keep to these rules, and one draw needn't show every extreme that they name: `tile_row`: each slot names one of its device's tile rows: d * 2 to d * 2 + 1 for device d. `tile_col`: each slot's tile column is (tile_row + o) mod 1024 with o from minus 2 to 2; no two slots of one device name the same pair of tile row and tile column. `tile_count`: some device has all 6 slots live.
All inputs are finite; a program needn't handle non-finite values.
Results may differ from the reference program's by a relative error of at most 0.0029.
Values may be sent and summed in bfloat16 or wider, within the bound.
No kernel may reach another device: no remote copies, remote signals or barrier semaphores. Data moves between devices by JAX's collectives and lax.ppermute only.
A program may use at most 64 MiB of HBM per device.

```python
import jax
import jax.numpy as jnp
from jax import lax

BS = 512
K = 256
TR = 2
H = 2
TILES_DEV = 6
NT = 1024
N = 524288
N_GRP = 8
N_ROW = 64


def slot_pairs(key):
    device_total = N_GRP * N_ROW
    span = 2 * H + 1
    pair_total = TR * span
    keys = jax.random.split(jax.random.fold_in(key, 31), device_total)
    scores = jax.vmap(lambda single: jax.random.permutation(single, pair_total))(keys).astype(jnp.int32)
    pair_ids = jnp.arange(pair_total, dtype=jnp.int32)[None, :]
    first_pair = H - 1
    second_pair = (TR - 1) * span + H + 1
    third_pair = H
    scores = jnp.where(pair_ids == first_pair, -3, jnp.where(pair_ids == second_pair, -2, jnp.where(pair_ids == third_pair, -1, scores)))
    order = jnp.argsort(scores, axis=1, stable=True)[:, :TILES_DEV].astype(jnp.int32)
    local_row = order // span
    offset = order % span - H
    device = jnp.arange(device_total, dtype=jnp.int32)[:, None]
    rows = device * TR + local_row
    cols = (rows + offset) % (TR * device_total)
    return (rows.reshape(-1).astype(jnp.int32), cols.reshape(-1).astype(jnp.int32))


def draw_tile_row(key, part):
    rows, cols = slot_pairs(key)
    return rows


def draw_tile_col(key, part):
    rows, cols = slot_pairs(key)
    return cols


def draw_tile_count(key, part):
    device_total = N_GRP * N_ROW
    counts = jax.random.randint(jax.random.fold_in(key, 21), (device_total,), 3, TILES_DEV + 1, dtype=jnp.int32)
    busiest = jax.random.randint(jax.random.fold_in(key, 22), (), 0, device_total, dtype=jnp.int32)
    device_ids = jnp.arange(device_total, dtype=jnp.int32)
    return jnp.where(device_ids == busiest, TILES_DEV, counts).astype(jnp.int32)


def draw_q_block(key, part):
    row_tile = jnp.arange(N, dtype=jnp.int32) // BS
    row_scale = 10.0 ** (row_tile.astype(jnp.float32) / (NT - 1))
    base = jnp.clip(jax.random.normal(jax.random.fold_in(key, 43), (N, K), jnp.float32), -6.0, 6.0)
    return (base * row_scale[:, None]).astype(jnp.bfloat16)


def steps_of(stream_key, dims, cuts, low, high):
    level = 1.0
    for position, shards_of in cuts:
        draws = jax.random.uniform(jax.random.fold_in(jax.random.fold_in(stream_key, 6), position), (shards_of,), jnp.float32, low / len(cuts), high / len(cuts))
        level = level * jnp.repeat(jnp.exp(draws), dims[position] // shards_of).reshape((-1,) + (1,) * (len(dims) - 1 - position))
    return level


def centred(rng, shape, deviation, reach, cuts=(), held_as=jnp.bfloat16):
    gain = steps_of(rng, shape, cuts, -0.22, 0.18) if cuts else 1.0
    array = jax.random.normal(rng, shape, jnp.float32) * deviation * gain
    return jnp.minimum(jnp.maximum(array, -reach), reach).astype(held_as)


def setup_inputs(seed: int = 0) -> dict:
    key_of = jax.random.split(jax.random.key(seed), 6)
    tiles = centred(key_of[0], (N_GRP * N_ROW * TILES_DEV, BS, BS), (BS * TILES_DEV // TR) ** -0.5, 0.15625, ((0, 512),))
    tile_row = draw_tile_row(jax.random.fold_in(key_of[5], 71), 0)
    tile_col = draw_tile_col(jax.random.fold_in(key_of[5], 71), 0)
    tile_count = draw_tile_count(jax.random.fold_in(key_of[5], 71), 0)
    q_block = draw_q_block(jax.random.fold_in(key_of[5], 71), 0)
    return dict(tiles=tiles, tile_row=tile_row, tile_col=tile_col, tile_count=tile_count, q_block=q_block)


def reference(tiles, tile_row, tile_col, tile_count, q_block):
    device_total = N_GRP * N_ROW
    tile_sets = tiles.reshape(device_total, TILES_DEV, BS, BS)
    slot_rows = tile_row.reshape(device_total, TILES_DEV)
    slot_cols = tile_col.reshape(device_total, TILES_DEV)
    q_tiles = q_block.astype(jnp.float32).reshape(NT, BS, K)
    slot_ids = jnp.arange(TILES_DEV, dtype=jnp.int32)
    row_ids = jnp.arange(TR, dtype=jnp.int32)
    column_ids = jnp.arange(TR + 2 * H, dtype=jnp.int32)

    def forward(device):
        live_slot = slot_ids < tile_count[device]
        local_row = (slot_rows[device] - device * TR).astype(jnp.int32)
        blocks = q_tiles[slot_cols[device]]
        products = jnp.einsum('sab,sbk->sak', tile_sets[device].astype(jnp.float32), blocks, precision=lax.Precision.HIGHEST)
        placing = ((local_row[None, :] == row_ids[:, None]) & live_slot[None, :]).astype(jnp.float32)
        return jnp.einsum('rs,sak->rak', placing, products, precision=lax.Precision.HIGHEST)
    aq_tiles = lax.map(forward, jnp.arange(device_total, dtype=jnp.int32)).reshape(NT, BS, K).astype(jnp.bfloat16)

    def backward(device):
        live_slot = slot_ids < tile_count[device]
        local_col = ((slot_cols[device] - device * TR + H) % NT).astype(jnp.int32)
        row_part = aq_tiles[slot_rows[device]].astype(jnp.float32)
        images = jnp.einsum('sab,sak->sbk', tile_sets[device].astype(jnp.float32), row_part, precision=lax.Precision.HIGHEST)
        placing = ((local_col[None, :] == column_ids[:, None]) & live_slot[None, :]).astype(jnp.float32)
        sums = jnp.einsum('cs,sbk->cbk', placing, images, precision=lax.Precision.HIGHEST)
        return (sums[H:H + TR], sums[:H].astype(jnp.bfloat16), sums[H + TR:].astype(jnp.bfloat16))
    own_part, lower, upper = lax.map(backward, jnp.arange(device_total, dtype=jnp.int32))
    lower, upper = lax.optimization_barrier((lower, upper))
    from_above = jnp.roll(lower, -1, axis=0).astype(jnp.float32)
    from_below = jnp.roll(upper, 1, axis=0).astype(jnp.float32)
    own_part = own_part.at[:, TR - H:].add(from_above)
    own_part = own_part.at[:, :H].add(from_below)
    y_full = own_part.reshape(N, K)
    gram_matrix = jnp.dot(y_full.T.astype(jnp.float32), y_full.astype(jnp.float32), precision=lax.Precision.HIGHEST, preferred_element_type=jnp.float32) / N
    factor_low = jnp.linalg.cholesky(gram_matrix)
    return lax.linalg.triangular_solve(factor_low, y_full, left_side=False, lower=True, transpose_a=True)
```

```python
import functools

import jax
import jax.numpy as jnp
from jax import lax
from jax.experimental import pallas as pl
from jax.experimental.pallas import tpu as pltpu
from jax.sharding import Mesh
from jax.sharding import PartitionSpec as P

H = 2
LEAF = 64
AXES = ("grp", "y", "x", "core")
F32 = jnp.float32
BF16 = jnp.bfloat16
HIGHEST = lax.Precision.HIGHEST


def dot(a, b, ca, cb, precision=None):
    return lax.dot_general(
        a, b, (((ca,), (cb,)), ((), ())), precision=precision, preferred_element_type=F32
    )


def band_kernel(
    nt, row_ref, col_ref, count_ref, tiles_ref, low_ref, q_ref, high_ref,
    own_ref, lower_ref, upper_ref, win, acc, terms, aq,
):
    slots, bs, _ = tiles_ref.shape
    own = q_ref.shape[0] // bs
    for c in range(H):
        win[c] = low_ref[pl.ds(c * bs, bs), :]
        win[H + own + c] = high_ref[pl.ds(c * bs, bs), :]
    for c in range(own):
        win[H + c] = q_ref[pl.ds(c * bs, bs), :]
    acc[...] = jnp.zeros_like(acc)
    terms[...] = jnp.zeros_like(terms)

    def place(s):
        row = row_ref[s]
        off = col_ref[s] - row + H
        off = jnp.where(off < 0, off + nt, off)
        off = jnp.where(off >= nt, off - nt, off)
        row = lax.rem(row, own)
        return row, row + off

    for s in range(slots):

        @pl.when(s < count_ref[0])
        def _():
            row, col = place(s)
            acc[row] += dot(tiles_ref[s], win[col], 1, 0)

    aq[...] = acc[...].astype(BF16)
    for s in range(slots):

        @pl.when(s < count_ref[0])
        def _():
            row, col = place(s)
            terms[col] += dot(tiles_ref[s], aq[row], 0, 0)

    for c in range(H):
        lower_ref[pl.ds(c * bs, bs), :] = terms[c].astype(BF16)
        upper_ref[pl.ds(c * bs, bs), :] = terms[H + own + c].astype(BF16)
    for c in range(own):
        own_ref[pl.ds(c * bs, bs), :] = terms[H + c]


def band(nt, tiles, tile_row, tile_col, tile_count, low, q, high):
    slots, bs, _ = tiles.shape
    rows, k = q.shape
    own = rows // bs
    smem = pl.BlockSpec(memory_space=pltpu.SMEM)
    vmem = pl.BlockSpec(memory_space=pltpu.VMEM)
    return pl.pallas_call(
        functools.partial(band_kernel, nt),
        out_shape=(
            jax.ShapeDtypeStruct((rows, k), F32),
            jax.ShapeDtypeStruct((H * bs, k), BF16),
            jax.ShapeDtypeStruct((H * bs, k), BF16),
        ),
        in_specs=[smem] * 3 + [vmem] * 4,
        out_specs=(vmem,) * 3,
        scratch_shapes=[
            pltpu.VMEM((own + 2 * H, bs, k), BF16),
            pltpu.VMEM((own, bs, k), F32),
            pltpu.VMEM((own + 2 * H, bs, k), F32),
            pltpu.VMEM((own, bs, k), BF16),
        ],
        compiler_params=pltpu.CompilerParams(vmem_limit_bytes=32 << 20),
        cost_estimate=pl.CostEstimate(
            flops=4 * slots * bs * bs * k, bytes_accessed=tiles.size * 2, transcendentals=0
        ),
        name="band",
    )(tile_row, tile_col, tile_count, tiles, low, q, high)


def gram_kernel(own_ref, below_ref, above_ref, y_ref, gram_ref):
    y = own_ref[...] + below_ref[...].astype(F32) + above_ref[...].astype(F32)
    y_ref[...] = y
    b = y.astype(BF16)
    half = b.shape[1] // 2
    full = dot(b, b, 0, 0)
    gram_ref[0:half, :] = full[:half, :half].astype(BF16)
    gram_ref[half : 2 * half, :] = full[:half, half:].astype(BF16)
    gram_ref[2 * half :, :] = full[half:, half:].astype(BF16)


def gram(own, below, above):
    rows, k = own.shape
    vmem = pl.BlockSpec(memory_space=pltpu.VMEM)
    return pl.pallas_call(
        gram_kernel,
        out_shape=(
            jax.ShapeDtypeStruct((rows, k), F32),
            jax.ShapeDtypeStruct((3 * k // 2, k // 2), BF16),
        ),
        in_specs=[vmem] * 3,
        out_specs=(vmem,) * 2,
        compiler_params=pltpu.CompilerParams(vmem_limit_bytes=32 << 20),
        cost_estimate=pl.CostEstimate(
            flops=2 * rows * k * k, bytes_accessed=8 * rows * k, transcendentals=0
        ),
        name="gram",
    )(own, below, above)


def spread(piece):
    return jnp.broadcast_to(piece, (8, 128))


def leaf_inverse(d):
    n = d.shape[0]
    pieces = n // 8
    eye = (
        lax.broadcasted_iota(jnp.int32, (n, n), 0) == lax.broadcasted_iota(jnp.int32, (n, n), 1)
    ).astype(F32)
    both = jnp.concatenate([eye, d], axis=1)
    a = [both[8 * r : 8 * r + 8, :] for r in range(pieces)]
    line = lax.broadcasted_iota(jnp.int32, (8, 128), 0)
    for t in range(pieces):
        cols = [
            [spread(a[r][:, n + 8 * t + i : n + 8 * t + i + 1]) for r in range(t, pieces)]
            for i in range(8)
        ]
        pivots = jnp.ones((8, 128), F32)
        for i in range(8):
            pivot = spread(cols[i][0][i : i + 1, :])
            pivots = jnp.where(line == i, pivot, pivots)
            root = lax.rsqrt(pivot)
            scale = root * root
            by = [c * scale for c in cols[i]]
            by[0] = jnp.where(line > i, by[0], 0.0)
            for j in range(i + 1, 8):
                row = spread(cols[j][0][i : i + 1, :])
                cols[j] = [c - b * row for c, b in zip(cols[j], by)]
            row = spread(a[t][i : i + 1, :])
            for r, b in enumerate(by):
                a[t + r] = a[t + r] - b * row
        a[t] = a[t] * lax.rsqrt(pivots)
    return jnp.concatenate([piece[:, :n] for piece in a], axis=0)


def factor_inverse(g):
    g11, g12, g22 = g
    x11 = whole_inverse(g11)
    b = dot(x11, g12, 1, 0, HIGHEST)
    s = g22 - dot(b, b, 0, 0, HIGHEST)
    x22 = whole_inverse(s)
    x21 = -dot(x22, dot(b, x11, 0, 0, HIGHEST), 1, 0, HIGHEST)
    return x11, x21, x22


def whole_inverse(d):
    n = d.shape[0]
    if n == LEAF:
        return leaf_inverse(d)
    h = n // 2
    x11, x21, x22 = factor_inverse((d[:h, :h], d[:h, h:], d[h:, h:]))
    upper = jnp.concatenate([x11, jnp.zeros_like(x11)], axis=1)
    return jnp.concatenate([upper, jnp.concatenate([x21, x22], axis=1)], axis=0)


def split(x):
    hi = x.astype(BF16)
    return hi, (x - hi.astype(F32)).astype(BF16)


def next_kernel(rows_total, gram_ref, y_ref, out_ref):
    half = gram_ref.shape[1]
    g = [gram_ref[pl.ds(i * half, half), :].astype(F32) / rows_total for i in range(3)]
    x11, x21, x22 = factor_inverse(g)
    upper = jnp.concatenate([x11, jnp.zeros_like(x11)], axis=1)
    x = jnp.concatenate([upper, jnp.concatenate([x21, x22], axis=1)], axis=0)
    x_hi, x_lo = split(x)
    y_hi, y_lo = split(y_ref[...])
    out_ref[...] = dot(y_hi, x_hi, 1, 1) + (dot(y_lo, x_hi, 1, 1) + dot(y_hi, x_lo, 1, 1))


def next_basis(rows_total, packed, y):
    rows, k = y.shape
    vmem = pl.BlockSpec(memory_space=pltpu.VMEM)
    return pl.pallas_call(
        functools.partial(next_kernel, rows_total),
        out_shape=jax.ShapeDtypeStruct((rows, k), F32),
        in_specs=[vmem] * 2,
        out_specs=vmem,
        compiler_params=pltpu.CompilerParams(vmem_limit_bytes=32 << 20),
        cost_estimate=pl.CostEstimate(
            flops=6 * rows * k * k, bytes_accessed=8 * rows * k, transcendentals=0
        ),
        name="next_basis",
    )(packed, y)


def summed(x):
    return x.astype(F32).sum(axis=0).astype(BF16)


def exchange(x, axes):
    return lax.all_to_all(x, axes, split_axis=0, concat_axis=0, tiled=True)


def from_everyone(x, axes):
    return exchange(jnp.broadcast_to(x, (lax.axis_size(axes), *x.shape)), axes)


def sum_everywhere(x):
    near = ("x", "core")
    parts = x.reshape(lax.axis_size(near), -1, x.shape[1])
    own = summed(exchange(parts, near))
    own = summed(from_everyone(own, "y"))
    own = summed(from_everyone(own, "grp"))
    return from_everyone(own, near).reshape(x.shape)


def on_device(tiles, tile_row, tile_col, tile_count, q_block):
    bs = tiles.shape[1]
    peers = lax.axis_size(AXES)
    rows = q_block.shape[0]
    up = [(i, (i + 1) % peers) for i in range(peers)]
    down = [(b, a) for a, b in up]
    low = lax.ppermute(q_block[rows - H * bs :], AXES, up)
    high = lax.ppermute(q_block[: H * bs], AXES, down)
    own, lower, upper = band(
        rows // bs * peers, tiles, tile_row, tile_col, tile_count, low, q_block, high
    )
    below = lax.ppermute(upper, AXES, up)
    above = lax.ppermute(lower, AXES, down)
    y, packed = gram(own, below, above)
    return next_basis(rows * peers, sum_everywhere(packed), y)


def solution(mesh):
    torus = Mesh(mesh.devices.reshape(mesh.shape["grp"], 8, 4, 2), AXES)
    return jax.shard_map(
        on_device,
        mesh=torus,
        in_specs=(P(AXES, None, None), P(AXES), P(AXES), P(AXES), P(AXES, None)),
        out_specs=P(AXES, None),
        check_vma=False,
    )
```

```python
import functools

import jax
import jax.numpy as jnp
from jax import lax
from jax.experimental import pallas as pl
from jax.experimental.pallas import tpu as pltpu
from jax.sharding import Mesh
from jax.sharding import PartitionSpec as P

H = 2
LEAF = 64
AXES = ("grp", "y", "x", "core")
F32 = jnp.float32
BF16 = jnp.bfloat16


def dot(a, b, ca, cb):
    return lax.dot_general(a, b, (((ca,), (cb,)), ((), ())), preferred_element_type=F32)


SMEM = pl.BlockSpec(memory_space=pltpu.SMEM)
VMEM = pl.BlockSpec(memory_space=pltpu.VMEM)
HBM = pl.BlockSpec(memory_space=pltpu.HBM)


class Slots:
    def __init__(self, table, slots, own, nt):
        self.table, self.slots, self.own, self.nt = table, slots, own, nt
        self.odd = lax.rem(lax.div(table[0], own), 2) == 1

    def live(self, s):
        return s < self.table[2 * self.slots]

    def row(self, s):
        return lax.rem(self.table[s], self.own)

    def column(self, s):
        off = self.table[self.slots + s] - self.table[s] + H
        off = jnp.where(off < 0, off + self.nt, off)
        off = jnp.where(off >= self.nt, off - self.nt, off)
        return self.row(s) + off

    def is_own(self, s):
        column = self.column(s)
        return jnp.logical_and(column >= H, column < H + self.own)

    def is_across(self, s):
        column = self.column(s)
        return jnp.where(self.odd, column >= H + self.own, column < H)

    def is_beside(self, s):
        column = self.column(s)
        return jnp.where(self.odd, column < H, column >= H + self.own)

    def in_side(self, s):
        column = self.column(s)
        return jnp.where(column < H, column, column - H - self.own)

    def in_own(self, s):
        return self.column(s) - H


def own_kernel(nt, table, tiles_ref, q_ref, held_ref, acc_ref, q_held, sems):
    slots = held_ref.shape[0]
    own = acc_ref.shape[0]
    at = Slots(table, slots, own, nt)
    copies = [pltpu.make_async_copy(q_ref, q_held, sems.at[slots])]
    copies += [
        pltpu.make_async_copy(tiles_ref.at[s], held_ref.at[s], sems.at[s]) for s in range(slots)
    ]
    for copy in copies:
        copy.start()
    acc_ref[...] = jnp.zeros_like(acc_ref)
    copies[0].wait()
    for s in range(slots):
        copies[s + 1].wait()

        @pl.when(jnp.logical_and(at.live(s), at.is_own(s)))
        def _():
            acc_ref[at.row(s)] += dot(held_ref[s], q_held[at.in_own(s)], 1, 0)


def across_kernel(nt, table, held_ref, acc_in, across_ref, beside_ref, aq_ref, out_ref, acc, terms):
    slots = held_ref.shape[0]
    at = Slots(table, slots, acc.shape[0], nt)
    acc[...] = acc_in[...]
    terms[...] = jnp.zeros_like(terms)
    for s in range(slots):
        for there, side in ((at.is_beside(s), beside_ref), (at.is_across(s), across_ref)):

            @pl.when(jnp.logical_and(at.live(s), there))
            def _(side=side):
                acc[at.row(s)] += dot(held_ref[s], side[at.in_side(s)], 1, 0)

    aq_ref[...] = acc[...].astype(BF16)
    for s in range(slots):

        @pl.when(jnp.logical_and(at.live(s), at.is_across(s)))
        def _():
            terms[at.in_side(s)] += dot(held_ref[s], aq_ref[at.row(s)], 0, 0)

    out_ref[...] = terms[...].astype(BF16)


def rest_kernel(nt, table, held_ref, aq_ref, out_ref, own_ref, terms):
    slots = held_ref.shape[0]
    at = Slots(table, slots, own_ref.shape[0], nt)
    terms[...] = jnp.zeros_like(terms)
    own_ref[...] = jnp.zeros_like(own_ref)
    for s in range(slots):
        for there, sums, place in (
            (at.is_beside(s), terms, at.in_side(s)),
            (at.is_own(s), own_ref, at.in_own(s)),
        ):

            @pl.when(jnp.logical_and(at.live(s), there))
            def _(sums=sums, place=place):
                sums[place] += dot(held_ref[s], aq_ref[at.row(s)], 0, 0)

    out_ref[...] = terms[...].astype(BF16)


def kernel_call(body, outs, ins, scratch, products, args):
    bs = args[1].shape[-1]
    flops = 2 * products * bs * bs * outs[-1].shape[-1]
    return pl.pallas_call(
        body,
        out_shape=tuple(outs),
        in_specs=ins,
        out_specs=(VMEM,) * len(outs),
        scratch_shapes=scratch,
        compiler_params=pltpu.CompilerParams(vmem_limit_bytes=24 << 20),
        cost_estimate=pl.CostEstimate(flops=flops, bytes_accessed=4 << 20, transcendentals=0),
    )(*args)


def exchanged(x, pairs, shape):
    return lax.ppermute(x, AXES, pairs).reshape(shape)


def band(tiles, tile_row, tile_col, tile_count, q):
    slots, bs, _ = tiles.shape
    rows, k = q.shape
    own = rows // bs
    peers = lax.axis_size(AXES)
    nt = own * peers
    beside = [(d, d + 1 - 2 * (d % 2)) for d in range(peers)]
    across = [(d, (d - 1 + 2 * (d % 2)) % peers) for d in range(peers)]
    side = (H, bs, k)
    held = jax.ShapeDtypeStruct(tiles.shape, BF16)
    sums = jax.ShapeDtypeStruct((own, bs, k), F32)
    rim = jax.ShapeDtypeStruct(side, BF16)
    table = jnp.concatenate([tile_row, tile_col, tile_count])
    q_across = exchanged(q, across, side)
    q_beside = exchanged(q, beside, side)
    held, acc = kernel_call(
        functools.partial(own_kernel, nt), [held, sums], [SMEM, HBM, HBM],
        [pltpu.VMEM((own, bs, k), BF16), pltpu.SemaphoreType.DMA((slots + 1,))],
        slots, (table, tiles, q.reshape(own, bs, k)),
    )
    aq, rim_across = kernel_call(
        functools.partial(across_kernel, nt),
        [jax.ShapeDtypeStruct((own, bs, k), BF16), rim], [SMEM] + [VMEM] * 4,
        [pltpu.VMEM((own, bs, k), F32), pltpu.VMEM(side, F32)],
        2 * slots, (table, held, acc, q_across, q_beside),
    )
    from_across = exchanged(rim_across, across, (rows, k))
    rim_beside, sums = kernel_call(
        functools.partial(rest_kernel, nt), [rim, sums], [SMEM] + [VMEM] * 2,
        [pltpu.VMEM(side, F32)],
        slots, (table, held, aq),
    )
    from_beside = exchanged(rim_beside, beside, (rows, k))
    return sums.reshape(rows, k), from_across, from_beside


def gram_kernel(own_ref, below_ref, above_ref, y_ref, gram_ref):
    y = own_ref[...] + below_ref[...].astype(F32) + above_ref[...].astype(F32)
    y_ref[...] = y
    b = y.astype(BF16)
    half = b.shape[1] // 2
    full = dot(b, b, 0, 0)
    gram_ref[0:half, :] = full[:half, :half].astype(BF16)
    gram_ref[half : 2 * half, :] = full[:half, half:].astype(BF16)
    gram_ref[2 * half :, :] = full[half:, half:].astype(BF16)


def gram(own, below, above):
    rows, k = own.shape
    vmem = pl.BlockSpec(memory_space=pltpu.VMEM)
    return pl.pallas_call(
        gram_kernel,
        out_shape=(
            jax.ShapeDtypeStruct((rows, k), F32),
            jax.ShapeDtypeStruct((3 * k // 2, k // 2), BF16),
        ),
        in_specs=[vmem] * 3,
        out_specs=(vmem,) * 2,
        compiler_params=pltpu.CompilerParams(vmem_limit_bytes=32 << 20),
        cost_estimate=pl.CostEstimate(
            flops=2 * rows * k * k, bytes_accessed=8 * rows * k, transcendentals=0
        ),
        name="gram",
    )(own, below, above)


def spread(piece):
    return jnp.broadcast_to(piece, (8, 128))


def leaf_inverse(d, zero):
    n = d.shape[0]
    pieces = n // 8
    eye = (
        lax.broadcasted_iota(jnp.int32, (n, n), 0) == lax.broadcasted_iota(jnp.int32, (n, n), 1)
    ).astype(F32)
    both = jnp.concatenate([eye, d], axis=1)
    a = [both[8 * r : 8 * r + 8, :] for r in range(pieces)]
    line = lax.broadcasted_iota(jnp.int32, (8, 128), 0)
    for t in range(pieces):
        cols = [
            [spread(a[r][:, n + 8 * t + i : n + 8 * t + i + 1]) for r in range(t, pieces)]
            for i in range(8)
        ]
        for col in cols:
            col[0] = col[0] + zero
        pivot = spread(cols[0][0][0:1, :])
        roots = jnp.ones((8, 128), F32)
        for i in range(8):
            root = lax.rsqrt(pivot)
            roots = jnp.where(line == i, root, roots)
            if i < 7:
                beside = spread(cols[i][0][i + 1 : i + 2, :]) * root
                pivot = spread(cols[i + 1][0][i + 1 : i + 2, :]) - beside * beside
            by = [c * root for c in cols[i]]
            for j in range(i + 1, 8):
                row = spread(cols[j][0][i : i + 1, :]) * root
                cols[j] = [c - b * row for c, b in zip(cols[j], by)]
            by[0] = jnp.where(line > i, by[0], 0.0)
            row = spread(a[t][i : i + 1, :]) * root
            for r, b in enumerate(by):
                a[t + r] = a[t + r] - b * row
        a[t] = a[t] * roots
    return jnp.concatenate([piece[:, :n] for piece in a], axis=0)


def split(x):
    hi = x.astype(BF16)
    return hi, (x - hi.astype(F32)).astype(BF16)


def dot3(a, b, ca, cb):
    a_hi, a_lo = split(a)
    b_hi, b_lo = split(b)
    return dot(a_hi, b_hi, ca, cb) + (dot(a_lo, b_hi, ca, cb) + dot(a_hi, b_lo, ca, cb))


def factor_inverse(g, zero):
    g11, g12, g22 = g
    x11 = whole_inverse(g11, zero)
    b = dot3(x11, g12, 1, 0)
    s = g22 - dot3(b, b, 0, 0)
    x22 = whole_inverse(s, zero)
    x21 = -dot3(x22, dot3(b, x11, 0, 0), 1, 0)
    return x11, x21, x22


def joined(x11, x21, x22):
    upper = jnp.concatenate([x11, jnp.zeros_like(x11)], axis=1)
    return jnp.concatenate([upper, jnp.concatenate([x21, x22], axis=1)], axis=0)


def whole_inverse(d, zero):
    n = d.shape[0]
    if n == LEAF:
        return leaf_inverse(d, zero)
    h = n // 2
    return joined(*factor_inverse((d[:h, :h], d[:h, h:], d[h:, h:]), zero))


def next_kernel(rows_total, gram_ref, y_ref, out_ref):
    half = gram_ref.shape[1]
    g = [gram_ref[pl.ds(i * half, half), :].astype(F32) / rows_total for i in range(3)]
    x = joined(*factor_inverse(g, y_ref[0:8, 0:128] * 0.0))
    out_ref[...] = dot3(y_ref[...], x, 1, 1)


def next_basis(rows_total, packed, y):
    rows, k = y.shape
    vmem = pl.BlockSpec(memory_space=pltpu.VMEM)
    return pl.pallas_call(
        functools.partial(next_kernel, rows_total),
        out_shape=jax.ShapeDtypeStruct((rows, k), F32),
        in_specs=[vmem] * 2,
        out_specs=vmem,
        compiler_params=pltpu.CompilerParams(vmem_limit_bytes=32 << 20),
        cost_estimate=pl.CostEstimate(
            flops=6 * rows * k * k, bytes_accessed=8 * rows * k, transcendentals=0
        ),
        name="next_basis",
    )(packed, y)


def summed(x):
    return x.astype(F32).sum(axis=0).astype(BF16)


def exchange(x, axes):
    return lax.all_to_all(x, axes, split_axis=0, concat_axis=0, tiled=True)


def from_everyone(x, axes):
    return exchange(jnp.broadcast_to(x, (lax.axis_size(axes), *x.shape)), axes)


def sum_everywhere(x):
    near = ("x", "core")
    parts = x.reshape(lax.axis_size(near), -1, x.shape[1])
    own = summed(exchange(parts, near))
    own = summed(from_everyone(own, "y"))
    own = summed(from_everyone(own, "grp"))
    return from_everyone(own, near).reshape(x.shape)


def on_device(tiles, tile_row, tile_col, tile_count, q_block):
    rows_total = q_block.shape[0] * lax.axis_size(AXES)
    y, packed = gram(*band(tiles, tile_row, tile_col, tile_count, q_block))
    return next_basis(rows_total, sum_everywhere(packed), y)


def solution(mesh):
    torus = Mesh(mesh.devices.reshape(mesh.shape["grp"], 8, 4, 2), AXES)
    return jax.shard_map(
        on_device,
        mesh=torus,
        in_specs=(P(AXES, None, None), P(AXES), P(AXES), P(AXES), P(AXES, None)),
        out_specs=P(AXES, None),
        check_vma=False,
    )
```

```python
import functools

import jax
import jax.numpy as jnp
from jax import lax
from jax.experimental import pallas as pl
from jax.experimental.pallas import tpu as pltpu
from jax.sharding import Mesh
from jax.sharding import PartitionSpec as P

H = 2
LEAF = 64
WIDTH = 16
AXES = ("z_high", "z_low", "y", "x", "core")
F32 = jnp.float32
BF16 = jnp.bfloat16


def dot(a, b, ca, cb):
    return lax.dot_general(a, b, (((ca,), (cb,)), ((), ())), preferred_element_type=F32)


SMEM = pl.BlockSpec(memory_space=pltpu.SMEM)
VMEM = pl.BlockSpec(memory_space=pltpu.VMEM)
HBM = pl.BlockSpec(memory_space=pltpu.HBM)


class Slots:
    def __init__(self, table, slots, own, nt):
        self.table, self.slots, self.own, self.nt = table, slots, own, nt
        self.odd = lax.rem(lax.div(table[0], own), 2) == 1

    def live(self, s):
        return s < self.table[2 * self.slots]

    def row(self, s):
        return lax.rem(self.table[s], self.own)

    def column(self, s):
        off = self.table[self.slots + s] - self.table[s] + H
        off = jnp.where(off < 0, off + self.nt, off)
        off = jnp.where(off >= self.nt, off - self.nt, off)
        return self.row(s) + off

    def is_own(self, s):
        column = self.column(s)
        return jnp.logical_and(column >= H, column < H + self.own)

    def is_across(self, s):
        column = self.column(s)
        return jnp.where(self.odd, column >= H + self.own, column < H)

    def is_beside(self, s):
        column = self.column(s)
        return jnp.where(self.odd, column < H, column >= H + self.own)

    def in_side(self, s):
        column = self.column(s)
        return jnp.where(column < H, column, column - H - self.own)

    def in_own(self, s):
        return self.column(s) - H


def near_kernel(nt, table, tiles_ref, q_ref, beside_ref, held_ref, acc_ref, q_held, sems):
    slots = held_ref.shape[0]
    own = acc_ref.shape[0]
    at = Slots(table, slots, own, nt)
    copies = [pltpu.make_async_copy(q_ref, q_held, sems.at[slots])]
    copies += [
        pltpu.make_async_copy(tiles_ref.at[s], held_ref.at[s], sems.at[s]) for s in range(slots)
    ]
    for copy in copies:
        copy.start()
    acc_ref[...] = jnp.zeros_like(acc_ref)
    copies[0].wait()
    for s in range(slots):
        copies[s + 1].wait()
        for there, side, place in (
            (at.is_own(s), q_held, at.in_own(s)),
            (at.is_beside(s), beside_ref, at.in_side(s)),
        ):

            @pl.when(jnp.logical_and(at.live(s), there))
            def _(side=side, place=place):
                acc_ref[at.row(s)] += dot(held_ref[s], side[place], 1, 0)


def across_kernel(nt, table, held_ref, acc_in, across_ref, aq_ref, out_ref, acc, terms):
    slots = held_ref.shape[0]
    at = Slots(table, slots, acc.shape[0], nt)
    acc[...] = acc_in[...]
    terms[...] = jnp.zeros_like(terms)
    for s in range(slots):

        @pl.when(jnp.logical_and(at.live(s), at.is_across(s)))
        def _():
            acc[at.row(s)] += dot(held_ref[s], across_ref[at.in_side(s)], 1, 0)

    aq_ref[...] = acc[...].astype(BF16)
    for s in range(slots):

        @pl.when(jnp.logical_and(at.live(s), at.is_across(s)))
        def _():
            terms[at.in_side(s)] += dot(held_ref[s], aq_ref[at.row(s)], 0, 0)

    out_ref[...] = terms[...].astype(BF16)


def rest_kernel(nt, table, held_ref, aq_ref, out_ref, own_ref, terms):
    slots = held_ref.shape[0]
    at = Slots(table, slots, own_ref.shape[0], nt)
    terms[...] = jnp.zeros_like(terms)
    own_ref[...] = jnp.zeros_like(own_ref)
    for s in range(slots):
        for there, sums, place in (
            (at.is_beside(s), terms, at.in_side(s)),
            (at.is_own(s), own_ref, at.in_own(s)),
        ):

            @pl.when(jnp.logical_and(at.live(s), there))
            def _(sums=sums, place=place):
                sums[place] += dot(held_ref[s], aq_ref[at.row(s)], 0, 0)

    out_ref[...] = terms[...].astype(BF16)


def kernel_call(body, outs, ins, scratch, products, args):
    bs = args[1].shape[-1]
    flops = 2 * products * bs * bs * outs[-1].shape[-1]
    return pl.pallas_call(
        body,
        out_shape=tuple(outs),
        in_specs=ins,
        out_specs=(VMEM,) * len(outs),
        scratch_shapes=scratch,
        compiler_params=pltpu.CompilerParams(vmem_limit_bytes=24 << 20),
        cost_estimate=pl.CostEstimate(flops=flops, bytes_accessed=4 << 20, transcendentals=0),
    )(*args)


def in_hbm(x):
    return pltpu.with_memory_space_constraint(x, pltpu.HBM)


def exchanged(x, pairs, shape):
    return lax.ppermute(x, AXES, pairs).reshape(shape)


def band(tiles, tile_row, tile_col, tile_count, q):
    slots, bs, _ = tiles.shape
    rows, k = q.shape
    own = rows // bs
    peers = lax.axis_size(AXES)
    nt = own * peers
    beside = [(d, d + 1 - 2 * (d % 2)) for d in range(peers)]
    across = [(d, (d - 1 + 2 * (d % 2)) % peers) for d in range(peers)]
    side = (H, bs, k)
    held = jax.ShapeDtypeStruct(tiles.shape, BF16)
    sums = jax.ShapeDtypeStruct((own, bs, k), F32)
    rim = jax.ShapeDtypeStruct(side, BF16)
    table = jnp.concatenate([tile_row, tile_col, tile_count])
    q_across = exchanged(q, across, side)
    q_beside = exchanged(q, beside, side)
    held, acc = kernel_call(
        functools.partial(near_kernel, nt), [held, sums], [SMEM, HBM, HBM, VMEM],
        [pltpu.VMEM((own, bs, k), BF16), pltpu.SemaphoreType.DMA((slots + 1,))],
        slots, (table, in_hbm(tiles), in_hbm(q.reshape(own, bs, k)), q_beside),
    )
    aq, rim_across = kernel_call(
        functools.partial(across_kernel, nt),
        [jax.ShapeDtypeStruct((own, bs, k), BF16), rim], [SMEM] + [VMEM] * 3,
        [pltpu.VMEM((own, bs, k), F32), pltpu.VMEM(side, F32)],
        slots, (table, held, acc, q_across),
    )
    from_across = exchanged(rim_across, across, (rows, k))
    rim_beside, sums = kernel_call(
        functools.partial(rest_kernel, nt), [rim, sums], [SMEM] + [VMEM] * 2,
        [pltpu.VMEM(side, F32)],
        slots, (table, held, aq),
    )
    from_beside = exchanged(rim_beside, beside, (rows, k))
    return sums.reshape(rows, k), from_across, from_beside


def gram_kernel(own_ref, below_ref, above_ref, y_ref, gram_ref):
    y = own_ref[...] + below_ref[...].astype(F32) + above_ref[...].astype(F32)
    y_ref[...] = y
    b = y.astype(BF16)
    half = b.shape[1] // 2
    full = dot(b, b, 0, 0)
    gram_ref[0:half, :] = full[:half, :half].astype(BF16)
    gram_ref[half : 2 * half, :] = full[:half, half:].astype(BF16)
    gram_ref[2 * half :, :] = full[half:, half:].astype(BF16)


def gram(own, below, above):
    rows, k = own.shape
    vmem = pl.BlockSpec(memory_space=pltpu.VMEM)
    return pl.pallas_call(
        gram_kernel,
        out_shape=(
            jax.ShapeDtypeStruct((rows, k), F32),
            jax.ShapeDtypeStruct((3 * k // 2, k // 2), BF16),
        ),
        in_specs=[vmem] * 3,
        out_specs=(vmem,) * 2,
        compiler_params=pltpu.CompilerParams(vmem_limit_bytes=32 << 20),
        cost_estimate=pl.CostEstimate(
            flops=2 * rows * k * k, bytes_accessed=8 * rows * k, transcendentals=0
        ),
        name="gram",
    )(own, below, above)


def spread(piece):
    return jnp.broadcast_to(piece, (8, 128))


def leaf_inverse(d, zero):
    n = d.shape[0]
    pieces = n // 8
    eye = (
        lax.broadcasted_iota(jnp.int32, (n, n), 0) == lax.broadcasted_iota(jnp.int32, (n, n), 1)
    ).astype(F32)
    both = jnp.concatenate([eye, d], axis=1)
    a = [both[8 * r : 8 * r + 8, :] for r in range(pieces)]
    line = lax.broadcasted_iota(jnp.int32, (8, 128), 0)
    for first in range(0, n, WIDTH):
        top = first // 8
        cols = [
            [spread(a[r][:, n + first + i : n + first + i + 1]) for r in range(top, pieces)]
            for i in range(WIDTH)
        ]
        for col in cols:
            col[0] = col[0] + zero
        pivot = spread(cols[0][0][0:1, :])
        roots = None
        for i in range(WIDTH):
            at, k = divmod(i, 8)
            root = lax.rsqrt(pivot)
            roots = root if k == 0 else jnp.where(line == k, root, roots)
            if i + 1 < WIDTH:
                p, q = divmod(i + 1, 8)
                beside = spread(cols[i][p][q : q + 1, :]) * root
                pivot = spread(cols[i + 1][p][q : q + 1, :]) - beside * beside
            by = [c * root for c in cols[i][at:]]
            for j in range(i + 1, WIDTH):
                row = spread(cols[j][at][k : k + 1, :]) * root
                cols[j] = cols[j][:at] + [c - b * row for c, b in zip(cols[j][at:], by)]
            row = spread(a[top + at][k : k + 1, :]) * root
            by[0] = jnp.where(line > k, by[0], 0.0)
            for r, b in enumerate(by):
                a[top + at + r] = a[top + at + r] - b * row
            if k == 7:
                a[top + at] = a[top + at] * roots
    return jnp.concatenate([piece[:, :n] for piece in a], axis=0)


def split(x):
    hi = x.astype(BF16)
    return hi, (x - hi.astype(F32)).astype(BF16)


def dot3(a, b, ca, cb):
    a_hi, a_lo = split(a)
    b_hi, b_lo = split(b)
    return dot(a_hi, b_hi, ca, cb) + (dot(a_lo, b_hi, ca, cb) + dot(a_hi, b_lo, ca, cb))


def factor_inverse(g, zero):
    g11, g12, g22 = g
    x11 = whole_inverse(g11, zero)
    b = dot3(x11, g12, 1, 0)
    s = g22 - dot3(b, b, 0, 0)
    x22 = whole_inverse(s, zero)
    x21 = -dot3(x22, dot3(b, x11, 0, 0), 1, 0)
    return x11, x21, x22


def joined(x11, x21, x22):
    upper = jnp.concatenate([x11, jnp.zeros_like(x11)], axis=1)
    return jnp.concatenate([upper, jnp.concatenate([x21, x22], axis=1)], axis=0)


def whole_inverse(d, zero):
    n = d.shape[0]
    if n == LEAF:
        return leaf_inverse(d, zero)
    h = n // 2
    return joined(*factor_inverse((d[:h, :h], d[:h, h:], d[h:, h:]), zero))


def next_kernel(rows_total, gram_ref, y_ref, out_ref):
    half = gram_ref.shape[1]
    g = [gram_ref[pl.ds(i * half, half), :].astype(F32) / rows_total for i in range(3)]
    x = joined(*factor_inverse(g, y_ref[0:8, 0:128] * 0.0))
    out_ref[...] = dot3(y_ref[...], x, 1, 1)


def next_basis(rows_total, packed, y):
    rows, k = y.shape
    vmem = pl.BlockSpec(memory_space=pltpu.VMEM)
    return pl.pallas_call(
        functools.partial(next_kernel, rows_total),
        out_shape=jax.ShapeDtypeStruct((rows, k), F32),
        in_specs=[vmem] * 2,
        out_specs=vmem,
        compiler_params=pltpu.CompilerParams(vmem_limit_bytes=32 << 20),
        cost_estimate=pl.CostEstimate(
            flops=6 * rows * k * k, bytes_accessed=8 * rows * k, transcendentals=0
        ),
        name="next_basis",
    )(packed, y)


def summed(x):
    return x.astype(F32).sum(axis=0).astype(BF16)


def exchange(x, axes):
    return lax.all_to_all(x, axes, split_axis=0, concat_axis=0, tiled=True)


def from_everyone(x, axes):
    return exchange(jnp.broadcast_to(x, (lax.axis_size(axes), *x.shape)), axes)


def sum_everywhere(x):
    near, far = ("z_low", "x", "core"), ("z_high", "y")
    parts = x.reshape(lax.axis_size(near), -1, x.shape[1])
    own = summed(exchange(parts, near))
    own = summed(from_everyone(own, far))
    return from_everyone(own, near).reshape(x.shape)


def on_device(tiles, tile_row, tile_col, tile_count, q_block):
    rows_total = q_block.shape[0] * lax.axis_size(AXES)
    y, packed = gram(*band(tiles, tile_row, tile_col, tile_count, q_block))
    return next_basis(rows_total, sum_everywhere(packed), y)


def solution(mesh):
    torus = Mesh(mesh.devices.reshape(mesh.shape["grp"] // 2, 2, 8, 4, 2), AXES)
    return jax.shard_map(
        on_device,
        mesh=torus,
        in_specs=(P(AXES, None, None), P(AXES), P(AXES), P(AXES), P(AXES, None)),
        out_specs=P(AXES, None),
        check_vma=False,
    )
```

```python
import functools

import jax
import jax.numpy as jnp
from jax import lax
from jax.experimental import pallas as pl
from jax.experimental.pallas import tpu as pltpu
from jax.sharding import Mesh
from jax.sharding import PartitionSpec as P

H = 2
LEAF = 64
WIDTH = 16
AXES = ("z_high", "z_low", "y", "x", "core")
F32 = jnp.float32
BF16 = jnp.bfloat16


def dot(a, b, ca, cb):
    return lax.dot_general(a, b, (((ca,), (cb,)), ((), ())), preferred_element_type=F32)


def split(x):
    hi = x.astype(BF16)
    return hi, (x - hi.astype(F32)).astype(BF16)


SMEM = pl.BlockSpec(memory_space=pltpu.SMEM)
VMEM = pl.BlockSpec(memory_space=pltpu.VMEM)
HBM = pl.BlockSpec(memory_space=pltpu.HBM)


class Slots:
    def __init__(self, table, slots, own, nt):
        self.table, self.slots, self.own, self.nt = table, slots, own, nt
        self.odd = lax.rem(lax.div(table[0], own), 2) == 1

    def live(self, s):
        return s < self.table[2 * self.slots]

    def row(self, s):
        return lax.rem(self.table[s], self.own)

    def column(self, s):
        off = self.table[self.slots + s] - self.table[s] + H
        off = jnp.where(off < 0, off + self.nt, off)
        off = jnp.where(off >= self.nt, off - self.nt, off)
        return self.row(s) + off

    def is_own(self, s):
        column = self.column(s)
        return jnp.logical_and(column >= H, column < H + self.own)

    def is_across(self, s):
        column = self.column(s)
        return jnp.where(self.odd, column >= H + self.own, column < H)

    def is_beside(self, s):
        column = self.column(s)
        return jnp.where(self.odd, column < H, column >= H + self.own)

    def in_side(self, s):
        column = self.column(s)
        return jnp.where(column < H, column, column - H - self.own)

    def in_own(self, s):
        return self.column(s) - H


def near_kernel(nt, table, tiles_ref, q_ref, beside_ref, held_ref, acc_ref, q_held, sems):
    slots = held_ref.shape[0]
    own = acc_ref.shape[0]
    at = Slots(table, slots, own, nt)
    copies = [pltpu.make_async_copy(q_ref, q_held, sems.at[slots])]
    copies += [
        pltpu.make_async_copy(tiles_ref.at[s], held_ref.at[s], sems.at[s]) for s in range(slots)
    ]
    for copy in copies:
        copy.start()
    acc_ref[...] = jnp.zeros_like(acc_ref)
    copies[0].wait()
    for s in range(slots):
        copies[s + 1].wait()
        for there, side, place in (
            (at.is_own(s), q_held, at.in_own(s)),
            (at.is_beside(s), beside_ref, at.in_side(s)),
        ):

            @pl.when(jnp.logical_and(at.live(s), there))
            def _(side=side, place=place):
                acc_ref[at.row(s)] += dot(held_ref[s], side[place], 1, 0)


def across_kernel(nt, table, held_ref, acc_in, across_ref, aq_ref, out_ref, acc, terms):
    slots = held_ref.shape[0]
    at = Slots(table, slots, acc.shape[0], nt)
    acc[...] = acc_in[...]
    terms[...] = jnp.zeros_like(terms)
    for s in range(slots):

        @pl.when(jnp.logical_and(at.live(s), at.is_across(s)))
        def _():
            acc[at.row(s)] += dot(held_ref[s], across_ref[at.in_side(s)], 1, 0)

    aq_ref[...] = acc[...].astype(BF16)
    for s in range(slots):

        @pl.when(jnp.logical_and(at.live(s), at.is_across(s)))
        def _():
            terms[at.in_side(s)] += dot(held_ref[s], aq_ref[at.row(s)], 0, 0)

    out_ref[...] = terms[...].astype(BF16)


def rest_kernel(nt, table, held_ref, aq_ref, out_ref, own_ref, terms):
    slots = held_ref.shape[0]
    at = Slots(table, slots, own_ref.shape[0], nt)
    terms[...] = jnp.zeros_like(terms)
    own_ref[...] = jnp.zeros_like(own_ref)
    for s in range(slots):
        for there, sums, place in (
            (at.is_beside(s), terms, at.in_side(s)),
            (at.is_own(s), own_ref, at.in_own(s)),
        ):

            @pl.when(jnp.logical_and(at.live(s), there))
            def _(sums=sums, place=place):
                sums[place] += dot(held_ref[s], aq_ref[at.row(s)], 0, 0)

    out_ref[...] = terms[...].astype(BF16)


def kernel_call(body, outs, ins, scratch, products, args):
    bs = args[1].shape[-1]
    flops = 2 * products * bs * bs * outs[-1].shape[-1]
    return pl.pallas_call(
        body,
        out_shape=tuple(outs),
        in_specs=ins,
        out_specs=(VMEM,) * len(outs),
        scratch_shapes=scratch,
        compiler_params=pltpu.CompilerParams(vmem_limit_bytes=24 << 20),
        cost_estimate=pl.CostEstimate(flops=flops, bytes_accessed=4 << 20, transcendentals=0),
    )(*args)


def in_hbm(x):
    return pltpu.with_memory_space_constraint(x, pltpu.HBM)


def exchanged(x, pairs, shape):
    return lax.ppermute(x, AXES, pairs).reshape(shape)


def band(tiles, tile_row, tile_col, tile_count, q):
    slots, bs, _ = tiles.shape
    rows, k = q.shape
    own = rows // bs
    peers = lax.axis_size(AXES)
    nt = own * peers
    beside = [(d, d + 1 - 2 * (d % 2)) for d in range(peers)]
    across = [(d, (d - 1 + 2 * (d % 2)) % peers) for d in range(peers)]
    side = (H, bs, k)
    held = jax.ShapeDtypeStruct(tiles.shape, BF16)
    sums = jax.ShapeDtypeStruct((own, bs, k), F32)
    rim = jax.ShapeDtypeStruct(side, BF16)
    table = jnp.concatenate([tile_row, tile_col, tile_count])
    q_across = exchanged(q, across, side)
    q_beside = exchanged(q, beside, side)
    held, acc = kernel_call(
        functools.partial(near_kernel, nt), [held, sums], [SMEM, HBM, HBM, VMEM],
        [pltpu.VMEM((own, bs, k), BF16), pltpu.SemaphoreType.DMA((slots + 1,))],
        slots, (table, in_hbm(tiles), in_hbm(q.reshape(own, bs, k)), q_beside),
    )
    aq, rim_across = kernel_call(
        functools.partial(across_kernel, nt),
        [jax.ShapeDtypeStruct((own, bs, k), BF16), rim], [SMEM] + [VMEM] * 3,
        [pltpu.VMEM((own, bs, k), F32), pltpu.VMEM(side, F32)],
        slots, (table, held, acc, q_across),
    )
    from_across = exchanged(rim_across, across, (rows, k))
    rim_beside, sums = kernel_call(
        functools.partial(rest_kernel, nt), [rim, sums], [SMEM] + [VMEM] * 2,
        [pltpu.VMEM(side, F32)],
        slots, (table, held, aq),
    )
    from_beside = exchanged(rim_beside, beside, (rows, k))
    return sums.reshape(rows, k), from_across, from_beside


def gram_kernel(own_ref, across_ref, beside_ref, hi_ref, lo_ref, y_ref, gram_ref):
    half = y_ref.shape[1]
    y = own_ref[...] + across_ref[...].astype(F32) + beside_ref[...].astype(F32)
    hi, lo = split(y[:, :half])
    hi_ref[...] = hi
    lo_ref[...] = lo
    y_ref[...] = y[:, half:]
    b = y.astype(BF16)
    full = dot(b, b, 0, 0)
    gram_ref[0:half, :] = full[:half, :half].astype(BF16)
    gram_ref[half : 2 * half, :] = full[half:, :half].astype(BF16)
    gram_ref[2 * half :, :] = full[half:, half:].astype(BF16)


def gram(own, across, beside):
    rows, k = own.shape
    return pl.pallas_call(
        gram_kernel,
        out_shape=(
            jax.ShapeDtypeStruct((rows, k // 2), BF16),
            jax.ShapeDtypeStruct((rows, k // 2), BF16),
            jax.ShapeDtypeStruct((rows, k // 2), F32),
            jax.ShapeDtypeStruct((3 * k // 2, k // 2), BF16),
        ),
        in_specs=[VMEM] * 3,
        out_specs=(VMEM,) * 4,
        compiler_params=pltpu.CompilerParams(vmem_limit_bytes=32 << 20),
        cost_estimate=pl.CostEstimate(
            flops=2 * rows * k * k, bytes_accessed=8 * rows * k, transcendentals=0
        ),
        name="gram",
    )(own, across, beside)


def spread(piece):
    return jnp.broadcast_to(piece, (8, 128))


def leaf_inverse(d, zero, left=None):
    n = d.shape[0]
    pieces = n // 8
    eye = (
        lax.broadcasted_iota(jnp.int32, (n, n), 0) == lax.broadcasted_iota(jnp.int32, (n, n), 1)
    ).astype(F32)
    wide = [jnp.concatenate([eye, d], axis=1)]
    if left is not None:
        wide.append(jnp.concatenate([left, left], axis=1))
    a = [[part[8 * r : 8 * r + 8, :] for part in wide] for r in range(pieces)]
    line = lax.broadcasted_iota(jnp.int32, (8, 128), 0)
    for first in range(0, n, WIDTH):
        top = first // 8

        cols = [
            [spread(a[r][0][:, n + first + i : n + first + i + 1]) for r in range(top, pieces)]
            for i in range(WIDTH)
        ]
        for col in cols:
            col[0] = col[0] + zero
        pivot = spread(cols[0][0][0:1, :])
        roots = None
        for i in range(WIDTH):
            at, k = divmod(i, 8)
            root = lax.rsqrt(pivot)
            roots = root if k == 0 else jnp.where(line == k, root, roots)
            if i + 1 < WIDTH:
                p, q = divmod(i + 1, 8)
                beside = spread(cols[i][p][q : q + 1, :]) * root
                pivot = spread(cols[i + 1][p][q : q + 1, :]) - beside * beside
            by = [c * root for c in cols[i][at:]]
            for j in range(i + 1, WIDTH):
                row = spread(cols[j][at][k : k + 1, :]) * root
                cols[j] = cols[j][:at] + [c - b * row for c, b in zip(cols[j][at:], by)]
            rows = [spread(part[k : k + 1, :]) * root for part in a[top + at]]
            by[0] = jnp.where(line > k, by[0], 0.0)
            for r, b in enumerate(by):
                a[top + at + r] = [p - b * row for p, row in zip(a[top + at + r], rows)]
            if k == 7:
                a[top + at] = [part * roots for part in a[top + at]]
    done = [jnp.concatenate([piece[i][:, :n] for piece in a], axis=0) for i in range(len(wide))]
    return done[0] if left is None else tuple(done)


def dot3(a, b, ca, cb):
    (a_hi, a_lo), (b_hi, b_lo) = a, b
    return dot(a_hi, b_hi, ca, cb) + (dot(a_lo, b_hi, ca, cb) + dot(a_hi, b_lo, ca, cb))


def eliminated(x11, d21, d22):
    x11 = split(x11)
    l21 = split(dot3(split(d21), x11, 1, 1))
    return x11, l21, d22 - dot3(l21, l21, 1, 1)


def factor_inverse(d, zero):
    h = LEAF
    x11 = leaf_inverse(d[:h, :h], zero)
    s11, l21, s = eliminated(x11, d[h:, :h], d[h:, h:])
    x22, x21 = leaf_inverse(s, zero, -dot3(l21, s11, 1, 0))
    upper = jnp.concatenate([x11, jnp.zeros_like(x11)], axis=1)
    return jnp.concatenate([upper, jnp.concatenate([x21, x22], axis=1)], axis=0)


CHUNKS = 4


def next_kernel(rows_total, gram_ref, hi_ref, lo_ref, y_ref, out_ref, first, second, rest, sems):
    half = gram_ref.shape[1]
    step = y_ref.shape[0] // CHUNKS
    d11, d21, d22 = (
        gram_ref[pl.ds(i * half, half), :].astype(F32) / rows_total for i in range(3)
    )
    zero = y_ref[0:8, 0:128] * 0.0
    x11, l21, s = eliminated(factor_inverse(d11, zero), d21, d22)
    q1 = dot3((hi_ref[...], lo_ref[...]), x11, 1, 1)
    first[...] = q1
    copies = [pltpu.make_async_copy(first, out_ref.at[:, pl.ds(0, half)], sems.at[CHUNKS])]
    copies[0].start()
    rest[0], rest[1] = split(y_ref[...] - dot3(split(q1), l21, 1, 1))
    x22 = split(factor_inverse(s, zero))
    for i in range(CHUNKS):
        rows = pl.ds(i * step, step)
        second[rows, :] = dot3((rest[0, rows, :], rest[1, rows, :]), x22, 1, 1)
        copy = pltpu.make_async_copy(
            second.at[rows], out_ref.at[rows, pl.ds(half, half)], sems.at[i]
        )
        copy.start()
        copies.append(copy)
    for copy in copies:
        copy.wait()


def next_basis(rows_total, packed, hi, lo, y):
    rows, half = y.shape
    return pl.pallas_call(
        functools.partial(next_kernel, rows_total),
        out_shape=jax.ShapeDtypeStruct((rows, 2 * half), F32),
        in_specs=[VMEM] * 4,
        out_specs=HBM,
        scratch_shapes=[
            pltpu.VMEM((rows, half), F32),
            pltpu.VMEM((rows, half), F32),
            pltpu.VMEM((2, rows, half), BF16),
            pltpu.SemaphoreType.DMA((CHUNKS + 1,)),
        ],
        compiler_params=pltpu.CompilerParams(vmem_limit_bytes=32 << 20),
        cost_estimate=pl.CostEstimate(
            flops=24 * rows * half * half, bytes_accessed=16 * rows * half, transcendentals=0
        ),
        name="next_basis",
    )(packed, hi, lo, y)


def summed(x):
    return x.astype(F32).sum(axis=0).astype(BF16)


def exchange(x, axes):
    return lax.all_to_all(x, axes, split_axis=0, concat_axis=0, tiled=True)


def from_everyone(x, axes):
    return exchange(jnp.broadcast_to(x, (lax.axis_size(axes), *x.shape)), axes)


def sum_everywhere(x):
    near, far = ("z_low", "x", "core"), ("z_high", "y")
    parts = x.reshape(lax.axis_size(near), -1, x.shape[1])
    own = summed(exchange(parts, near))
    own = summed(from_everyone(own, far))
    return from_everyone(own, near).reshape(x.shape)


def on_device(tiles, tile_row, tile_col, tile_count, q_block):
    rows_total = q_block.shape[0] * lax.axis_size(AXES)
    hi, lo, y, packed = gram(*band(tiles, tile_row, tile_col, tile_count, q_block))
    return next_basis(rows_total, sum_everywhere(packed), hi, lo, y)


def solution(mesh):
    torus = Mesh(mesh.devices.reshape(mesh.shape["grp"] // 2, 2, 8, 4, 2), AXES)
    return jax.shard_map(
        on_device,
        mesh=torus,
        in_specs=(P(AXES, None, None), P(AXES), P(AXES), P(AXES), P(AXES, None)),
        out_specs=P(AXES, None),
        check_vma=False,
    )
```

```python
import functools

import jax
import jax.numpy as jnp
from jax import lax
from jax.experimental import pallas as pl
from jax.experimental.pallas import tpu as pltpu
from jax.sharding import Mesh
from jax.sharding import PartitionSpec as P

H = 2
LEAF = 64
WIDTH = 16
AXES = ("z", "y_high", "y_low", "x", "core")
F32 = jnp.float32
BF16 = jnp.bfloat16


def dot(a, b, ca, cb):
    return lax.dot_general(a, b, (((ca,), (cb,)), ((), ())), preferred_element_type=F32)


def split(x):
    hi = x.astype(BF16)
    return hi, (x - hi.astype(F32)).astype(BF16)


SMEM = pl.BlockSpec(memory_space=pltpu.SMEM)
VMEM = pl.BlockSpec(memory_space=pltpu.VMEM)
HBM = pl.BlockSpec(memory_space=pltpu.HBM)


class Slots:
    def __init__(self, table, slots, own, nt):
        self.table, self.slots, self.own, self.nt = table, slots, own, nt
        self.odd = lax.rem(lax.div(table[0], own), 2) == 1

    def live(self, s):
        return s < self.table[2 * self.slots]

    def row(self, s):
        return lax.rem(self.table[s], self.own)

    def column(self, s):
        off = self.table[self.slots + s] - self.table[s] + H
        off = jnp.where(off < 0, off + self.nt, off)
        off = jnp.where(off >= self.nt, off - self.nt, off)
        return self.row(s) + off

    def is_own(self, s):
        column = self.column(s)
        return jnp.logical_and(column >= H, column < H + self.own)

    def is_across(self, s):
        column = self.column(s)
        return jnp.where(self.odd, column >= H + self.own, column < H)

    def is_beside(self, s):
        column = self.column(s)
        return jnp.where(self.odd, column < H, column >= H + self.own)

    def in_side(self, s):
        column = self.column(s)
        return jnp.where(column < H, column, column - H - self.own)

    def in_own(self, s):
        return self.column(s) - H


def near_kernel(nt, table, tiles_ref, q_ref, beside_ref, held_ref, acc_ref, q_held, sems):
    slots = held_ref.shape[0]
    own = acc_ref.shape[0]
    at = Slots(table, slots, own, nt)
    copies = [pltpu.make_async_copy(q_ref, q_held, sems.at[slots])]
    copies += [
        pltpu.make_async_copy(tiles_ref.at[s], held_ref.at[s], sems.at[s]) for s in range(slots)
    ]
    for copy in copies:
        copy.start()
    acc_ref[...] = jnp.zeros_like(acc_ref)
    copies[0].wait()
    for s in range(slots):
        copies[s + 1].wait()
        for there, side, place in (
            (at.is_own(s), q_held, at.in_own(s)),
            (at.is_beside(s), beside_ref, at.in_side(s)),
        ):

            @pl.when(jnp.logical_and(at.live(s), there))
            def _(side=side, place=place):
                acc_ref[at.row(s)] += dot(held_ref[s], side[place], 1, 0)


def across_kernel(nt, table, held_ref, acc_in, across_ref, aq_ref, out_ref, acc, terms):
    slots = held_ref.shape[0]
    at = Slots(table, slots, acc.shape[0], nt)
    acc[...] = acc_in[...]
    terms[...] = jnp.zeros_like(terms)
    for s in range(slots):

        @pl.when(jnp.logical_and(at.live(s), at.is_across(s)))
        def _():
            acc[at.row(s)] += dot(held_ref[s], across_ref[at.in_side(s)], 1, 0)

    aq_ref[...] = acc[...].astype(BF16)
    for s in range(slots):

        @pl.when(jnp.logical_and(at.live(s), at.is_across(s)))
        def _():
            terms[at.in_side(s)] += dot(held_ref[s], aq_ref[at.row(s)], 0, 0)

    out_ref[...] = terms[...].astype(BF16)


def rest_kernel(nt, table, held_ref, aq_ref, out_ref, own_ref, terms):
    slots = held_ref.shape[0]
    at = Slots(table, slots, own_ref.shape[0], nt)
    terms[...] = jnp.zeros_like(terms)
    own_ref[...] = jnp.zeros_like(own_ref)
    for s in range(slots):
        for there, sums, place in (
            (at.is_beside(s), terms, at.in_side(s)),
            (at.is_own(s), own_ref, at.in_own(s)),
        ):

            @pl.when(jnp.logical_and(at.live(s), there))
            def _(sums=sums, place=place):
                sums[place] += dot(held_ref[s], aq_ref[at.row(s)], 0, 0)

    out_ref[...] = terms[...].astype(BF16)


def kernel_call(body, outs, ins, scratch, products, args):
    bs = args[1].shape[-1]
    flops = 2 * products * bs * bs * outs[-1].shape[-1]
    return pl.pallas_call(
        body,
        out_shape=tuple(outs),
        in_specs=ins,
        out_specs=(VMEM,) * len(outs),
        scratch_shapes=scratch,
        compiler_params=pltpu.CompilerParams(vmem_limit_bytes=24 << 20),
        cost_estimate=pl.CostEstimate(flops=flops, bytes_accessed=4 << 20, transcendentals=0),
    )(*args)


def in_hbm(x):
    return pltpu.with_memory_space_constraint(x, pltpu.HBM)


def exchanged(x, pairs, shape):
    return lax.ppermute(x, AXES, pairs).reshape(shape)


def band(tiles, tile_row, tile_col, tile_count, q):
    slots, bs, _ = tiles.shape
    rows, k = q.shape
    own = rows // bs
    peers = lax.axis_size(AXES)
    nt = own * peers
    beside = [(d, d + 1 - 2 * (d % 2)) for d in range(peers)]
    across = [(d, (d - 1 + 2 * (d % 2)) % peers) for d in range(peers)]
    side = (H, bs, k)
    held = jax.ShapeDtypeStruct(tiles.shape, BF16)
    sums = jax.ShapeDtypeStruct((own, bs, k), F32)
    rim = jax.ShapeDtypeStruct(side, BF16)
    table = jnp.concatenate([tile_row, tile_col, tile_count])
    q_across = exchanged(q, across, side)
    q_beside = exchanged(q, beside, side)
    held, acc = kernel_call(
        functools.partial(near_kernel, nt), [held, sums], [SMEM, HBM, HBM, VMEM],
        [pltpu.VMEM((own, bs, k), BF16), pltpu.SemaphoreType.DMA((slots + 1,))],
        slots, (table, in_hbm(tiles), in_hbm(q.reshape(own, bs, k)), q_beside),
    )
    aq, rim_across = kernel_call(
        functools.partial(across_kernel, nt),
        [jax.ShapeDtypeStruct((own, bs, k), BF16), rim], [SMEM] + [VMEM] * 3,
        [pltpu.VMEM((own, bs, k), F32), pltpu.VMEM(side, F32)],
        slots, (table, held, acc, q_across),
    )
    from_across = exchanged(rim_across, across, (rows, k))
    rim_beside, sums = kernel_call(
        functools.partial(rest_kernel, nt), [rim, sums], [SMEM] + [VMEM] * 2,
        [pltpu.VMEM(side, F32)],
        slots, (table, held, aq),
    )
    from_beside = exchanged(rim_beside, beside, (rows, k))
    return sums.reshape(rows, k), from_across, from_beside


def gram_kernel(own_ref, across_ref, beside_ref, hi_ref, lo_ref, y_ref, gram_ref):
    half = y_ref.shape[1]
    y = own_ref[...] + across_ref[...].astype(F32) + beside_ref[...].astype(F32)
    hi, lo = split(y[:, :half])
    hi_ref[...] = hi
    lo_ref[...] = lo
    y_ref[...] = y[:, half:]
    b = y.astype(BF16)
    full = dot(b, b, 0, 0)
    gram_ref[0:half, :] = full[:half, :half].astype(BF16)
    gram_ref[half : 2 * half, :] = full[half:, :half].astype(BF16)
    gram_ref[2 * half :, :] = full[half:, half:].astype(BF16)


def gram(own, across, beside):
    rows, k = own.shape
    return pl.pallas_call(
        gram_kernel,
        out_shape=(
            jax.ShapeDtypeStruct((rows, k // 2), BF16),
            jax.ShapeDtypeStruct((rows, k // 2), BF16),
            jax.ShapeDtypeStruct((rows, k // 2), F32),
            jax.ShapeDtypeStruct((3 * k // 2, k // 2), BF16),
        ),
        in_specs=[VMEM] * 3,
        out_specs=(VMEM,) * 4,
        compiler_params=pltpu.CompilerParams(vmem_limit_bytes=32 << 20),
        cost_estimate=pl.CostEstimate(
            flops=2 * rows * k * k, bytes_accessed=8 * rows * k, transcendentals=0
        ),
        name="gram",
    )(own, across, beside)


def spread(piece):
    return jnp.broadcast_to(piece, (8, 128))


def leaf_inverse(d, zero, left=None):
    n = d.shape[0]
    pieces = n // 8
    eye = (
        lax.broadcasted_iota(jnp.int32, (n, n), 0) == lax.broadcasted_iota(jnp.int32, (n, n), 1)
    ).astype(F32)
    wide = [jnp.concatenate([eye, d], axis=1)]
    if left is not None:
        wide.append(jnp.concatenate([left, left], axis=1))
    a = [[part[8 * r : 8 * r + 8, :] for part in wide] for r in range(pieces)]
    line = lax.broadcasted_iota(jnp.int32, (8, 128), 0)
    for first in range(0, n, WIDTH):
        top = first // 8

        cols = [
            [spread(a[r][0][:, n + first + i : n + first + i + 1]) for r in range(top, pieces)]
            for i in range(WIDTH)
        ]
        for col in cols:
            col[0] = col[0] + zero
        pivot = spread(cols[0][0][0:1, :])
        roots = None
        for i in range(WIDTH):
            at, k = divmod(i, 8)
            root = lax.rsqrt(pivot)
            roots = root if k == 0 else jnp.where(line == k, root, roots)
            if i + 1 < WIDTH:
                p, q = divmod(i + 1, 8)
                beside = spread(cols[i][p][q : q + 1, :]) * root
                pivot = spread(cols[i + 1][p][q : q + 1, :]) - beside * beside
            by = [c * root for c in cols[i][at:]]
            for j in range(i + 1, WIDTH):
                row = spread(cols[j][at][k : k + 1, :]) * root
                cols[j] = cols[j][:at] + [c - b * row for c, b in zip(cols[j][at:], by)]
            rows = [spread(part[k : k + 1, :]) * root for part in a[top + at]]
            by[0] = jnp.where(line > k, by[0], 0.0)
            for r, b in enumerate(by):
                a[top + at + r] = [p - b * row for p, row in zip(a[top + at + r], rows)]
            if k == 7:
                a[top + at] = [part * roots for part in a[top + at]]
    done = [jnp.concatenate([piece[i][:, :n] for piece in a], axis=0) for i in range(len(wide))]
    return done[0] if left is None else tuple(done)


def dot3(a, b, ca, cb):
    (a_hi, a_lo), (b_hi, b_lo) = a, b
    return dot(a_hi, b_hi, ca, cb) + (dot(a_lo, b_hi, ca, cb) + dot(a_hi, b_lo, ca, cb))


def eliminated(x11, d21, d22):
    x11 = split(x11)
    l21 = split(dot3(split(d21), x11, 1, 1))
    return x11, l21, d22 - dot3(l21, l21, 1, 1)


def factor_inverse(d, zero):
    h = LEAF
    x11 = leaf_inverse(d[:h, :h], zero)
    s11, l21, s = eliminated(x11, d[h:, :h], d[h:, h:])
    x22, x21 = leaf_inverse(s, zero, -dot3(l21, s11, 1, 0))
    upper = jnp.concatenate([x11, jnp.zeros_like(x11)], axis=1)
    return jnp.concatenate([upper, jnp.concatenate([x21, x22], axis=1)], axis=0)


CHUNKS = 4


def next_kernel(rows_total, gram_ref, hi_ref, lo_ref, y_ref, out_ref, first, second, rest, sems):
    half = gram_ref.shape[1]
    step = y_ref.shape[0] // CHUNKS
    d11, d21, d22 = (
        gram_ref[pl.ds(i * half, half), :].astype(F32) / rows_total for i in range(3)
    )
    zero = y_ref[0:8, 0:128] * 0.0
    x11, l21, s = eliminated(factor_inverse(d11, zero), d21, d22)
    q1 = dot3((hi_ref[...], lo_ref[...]), x11, 1, 1)
    first[...] = q1
    copies = [pltpu.make_async_copy(first, out_ref.at[:, pl.ds(0, half)], sems.at[CHUNKS])]
    copies[0].start()
    rest[0], rest[1] = split(y_ref[...] - dot3(split(q1), l21, 1, 1))
    x22 = split(factor_inverse(s, zero))
    for i in range(CHUNKS):
        rows = pl.ds(i * step, step)
        second[rows, :] = dot3((rest[0, rows, :], rest[1, rows, :]), x22, 1, 1)
        copy = pltpu.make_async_copy(
            second.at[rows], out_ref.at[rows, pl.ds(half, half)], sems.at[i]
        )
        copy.start()
        copies.append(copy)
    for copy in copies:
        copy.wait()


def next_basis(rows_total, packed, hi, lo, y):
    rows, half = y.shape
    return pl.pallas_call(
        functools.partial(next_kernel, rows_total),
        out_shape=jax.ShapeDtypeStruct((rows, 2 * half), F32),
        in_specs=[VMEM] * 4,
        out_specs=HBM,
        scratch_shapes=[
            pltpu.VMEM((rows, half), F32),
            pltpu.VMEM((rows, half), F32),
            pltpu.VMEM((2, rows, half), BF16),
            pltpu.SemaphoreType.DMA((CHUNKS + 1,)),
        ],
        compiler_params=pltpu.CompilerParams(vmem_limit_bytes=32 << 20),
        cost_estimate=pl.CostEstimate(
            flops=24 * rows * half * half, bytes_accessed=16 * rows * half, transcendentals=0
        ),
        name="next_basis",
    )(packed, hi, lo, y)


def summed(x):
    return x.astype(F32).sum(axis=0).astype(BF16)


def exchange(x, axes):
    return lax.all_to_all(x, axes, split_axis=0, concat_axis=0, tiled=True)


def from_everyone(x, axes):
    return exchange(jnp.broadcast_to(x, (lax.axis_size(axes), *x.shape)), axes)


def sum_everywhere(x):
    near, far = ("y_low", "x", "core"), ("z", "y_high")
    parts = x.reshape(lax.axis_size(near), -1, x.shape[1])
    own = summed(exchange(parts, near))
    own = summed(from_everyone(own, far))
    return from_everyone(own, near).reshape(x.shape)


def on_device(tiles, tile_row, tile_col, tile_count, q_block):
    rows_total = q_block.shape[0] * lax.axis_size(AXES)
    hi, lo, y, packed = gram(*band(tiles, tile_row, tile_col, tile_count, q_block))
    return next_basis(rows_total, sum_everywhere(packed), hi, lo, y)


def solution(mesh):
    torus = Mesh(mesh.devices.reshape(mesh.shape["grp"], 4, 2, 4, 2), AXES)
    return jax.shard_map(
        on_device,
        mesh=torus,
        in_specs=(P(AXES, None, None), P(AXES), P(AXES), P(AXES), P(AXES, None)),
        out_specs=P(AXES, None),
        check_vma=False,
    )
```
